32 devices in a mesh: dp: 2 (over x), expert: 16 (over z, y, core).
Axes of the slice: x: 2, y: 2, z: 4, core: 2. Of those that a mesh axis runs over, the one named last changes fastest.
Arguments:
- grad_out: bfloat16 [2048, 7168], P('expert', 'dp'), may hold values from -6 to 6
- expert_ids: int32 [2048, 8], P('expert'), may hold values from 0 to 15, all different within a row; in each aligned block of 128 rows (0 to 127, 128 to 255, ...) at most 80 rows name the same one
- keep: int32 [2048, 8], P('expert'), may hold values 0 or 1
- router_logits: float32 [2048, 8], P('expert'), may hold values from -6 to 6
- w_gate: bfloat16 [16, 7168, 1024], P('expert', 'dp'), may hold values from -0.0625 to 0.0625
- w_up: bfloat16 [16, 7168, 1024], P('expert', 'dp'), may hold values from -0.0625 to 0.0625
- w_down: bfloat16 [16, 1024, 7168], P('expert', None, 'dp'), may hold values from -0.1875 to 0.1875
- saved_gate: bfloat16 [16, 1024, 1280], P('expert', 'dp'), may hold values from -6 to 6
- saved_up: bfloat16 [16, 1024, 1280], P('expert', 'dp'), may hold values from -6 to 6
Outputs:
- grad_tokens: bfloat16 [2048, 7168], P('expert', 'dp')
- router_grad: float32 [2048, 8], P('expert')
The draws below stay inside these ranges and needn't reach their ends.
Inputs may be any that keep to these rules, and one draw needn't show every extreme that they name: `expert_ids`: each token names 8 different experts; the copies that one source's 128 tokens send to one expert number at most 80, and exactly 80 for some source and expert.
All inputs are finite; a program needn't handle non-finite values. No bound on the sum of `keep` on one device may be relied on, other than what follows from the above.
Results may differ from the reference program's by a relative error of at most 0.0065.
Values may be sent and summed in bfloat16 or wider, within the bound.
A program may use at most 128 MiB of HBM per device.

```python
import math
import jax
import jax.numpy as jnp
import numpy as np
from jax import lax

D = 7168
FF = 1024
K = 8
TOK_DEV = 128
EXPERTS = 16
TOKENS = 2048
CAP = 80
SLOTS = 1280
N_EXPERT = 16


def plant(result, rng, low, top_value):
    dims = result.shape
    spot = [jax.random.randint(jax.random.fold_in(rng, axis), (), 0, dims[axis]) for axis in range(len(dims))]
    result = result.at[tuple(spot)].set(low)
    longest = dims.index(max(dims))
    spot[longest] = (spot[longest] + 1) % dims[longest]
    return result.at[tuple(spot)].set(top_value)


def levels(own_key, dims, shards, low, largest):
    loudness = 1.0
    for position, blocks in shards:
        steps = jax.random.uniform(jax.random.fold_in(jax.random.fold_in(own_key, 6), position), (blocks,), jnp.float32, low / len(shards), largest / len(shards))
        loudness = loudness * jnp.repeat(jnp.exp(steps), dims[position] // blocks).reshape((-1,) + (1,) * (len(dims) - 1 - position))
    return loudness


def deal_out(key, own, number, rows, amount, top, most, skew):
    ranking = jax.random.permutation(key, amount)
    packed, usual = shares(amount, rows * top, most, skew, True), shares(amount, rows * top, most, skew, False)
    places = jnp.arange(amount)

    def named(tallies, offset_by):
        used = int((tallies > 0).sum())
        fixed = max(1, used // 4)
        passed = fixed + (places - fixed + offset_by * (used - fixed)) % max(1, amount - fixed)
        return jnp.zeros((amount,), jnp.int32).at[ranking[jnp.where(places < fixed, places, passed)]].set(jnp.asarray(tallies, jnp.int32))

    tallies = jnp.where(number % 4 == 0, named(packed, number // 4), named(usual, number - number // 4 - 1))
    mixed = jax.random.permutation(jax.random.fold_in(own, 3), amount)
    giver, receiver = mixed[0:amount // 2 * 2:2], mixed[1:amount // 2 * 2:2]
    margin = jnp.minimum(tallies[giver] - 1, most - tallies[receiver]) // 2
    margin = jnp.where((giver == ranking[0]) | (receiver == ranking[0]) | (tallies[receiver] == 0), 0, jnp.maximum(margin, 0))
    passed = jax.random.randint(jax.random.fold_in(own, 4), (amount // 2,), 0, 1 << 20) % (margin + 1)
    tallies = tallies.at[giver].add(-passed).at[receiver].add(passed)
    members = jnp.searchsorted(jnp.cumsum(tallies), jnp.arange(rows * top), side="right").astype(jnp.int32)
    listing = members.reshape(top, rows).T
    listing = listing[jax.random.permutation(jax.random.fold_in(own, 1), rows)]
    offset_by = jax.random.randint(jax.random.fold_in(own, 2), (rows, 1), 0, top)
    return jnp.take_along_axis(listing, (jnp.arange(top)[None, :] + offset_by) % top, axis=1)


def shares(amount, total, bound, lean, full):
    loads = [(1 << 20) // math.isqrt(grade ** lean) + 1 for grade in range(1, amount + 1)]
    largest = bound if full else min(bound, max(-(-total // amount), total * loads[0] // sum(loads)))
    least = 1 if total - largest >= amount - 1 else 0
    given, spare = [largest] + [least] * (amount - 1), total - largest - least * (amount - 1)
    while spare > 0:
        free = [i for i in range(1, amount) if given[i] < largest] or [i for i in range(1, amount) if given[i] < bound]
        pool, left = sum([loads[i] for i in free]), spare
        for i in free:
            extra = min(bound - given[i], max(1, left * loads[i] // pool), spare)
            given[i] = given[i] + extra
            spare = spare - extra
    return np.array(given)


def bell_draw(own_key, extent, spread, limit, cuts=(), held_as=jnp.bfloat16):
    level = levels(own_key, extent, cuts, -0.22, 0.18) if cuts else 1.0
    drawn = jax.random.normal(own_key, extent, jnp.float32) * spread * level
    return jnp.minimum(jnp.maximum(drawn, -limit), limit).astype(held_as)


def setup_inputs(seed: int = 0) -> dict:
    seeds = jax.random.split(jax.random.key(seed), 10)
    grad_out = bell_draw(seeds[0], (TOKENS, D), 1.0, 6.0, ((0, 16), (1, 2)))
    expert_ids_keys = jax.random.split(jax.random.fold_in(seeds[1], 1), TOKENS // TOK_DEV)
    expert_ids_turns = jax.random.permutation(jax.random.fold_in(seeds[1], 3), TOKENS // TOK_DEV)
    expert_ids = jax.vmap(lambda own, number: deal_out(jax.random.fold_in(seeds[1], 2), own, number, TOK_DEV, EXPERTS, K, CAP, 2))(expert_ids_keys, expert_ids_turns).reshape((TOKENS, K))
    keep = plant((jax.random.randint(seeds[2], (TOKENS, K), 0, 4) < 3).astype(jnp.int32), jax.random.fold_in(seeds[2], 1), 0, 1)
    router_logits = bell_draw(seeds[3], (TOKENS, K), 1.5, 6.0, ((0, 16),), jnp.float32)
    w_gate = bell_draw(seeds[4], (EXPERTS, D, FF), D ** -0.5, 0.0625, ((0, 16), (1, 2)))
    w_up = bell_draw(seeds[5], (EXPERTS, D, FF), D ** -0.5, 0.0625, ((0, 16), (1, 2)))
    w_down = bell_draw(seeds[6], (EXPERTS, FF, D), FF ** -0.5, 0.1875, ((0, 16), (2, 2)))
    saved_gate = bell_draw(seeds[7], (EXPERTS, FF, SLOTS), 1.5, 6.0, ((0, 16), (1, 2)))
    saved_up = bell_draw(seeds[8], (EXPERTS, FF, SLOTS), 1.0, 6.0, ((0, 16), (1, 2)))
    return dict(grad_out=grad_out, expert_ids=expert_ids, keep=keep, router_logits=router_logits, w_gate=w_gate, w_up=w_up, w_down=w_down, saved_gate=saved_gate, saved_up=saved_up)


routed_scale = 2.5


def positions(ids_block):
    onehot = (ids_block[:, None] == jnp.arange(EXPERTS, dtype=jnp.int32)[None, :]).astype(jnp.int32)
    earlier = jnp.cumsum(onehot, axis=0) - onehot
    return jnp.sum(earlier * onehot, axis=1).astype(jnp.int32)


def reference(grad_out, expert_ids, keep, router_logits, w_gate, w_up, w_down, saved_gate, saved_up):
    ids = expert_ids.reshape(N_EXPERT, TOK_DEV * K).astype(jnp.int32)
    slot = jax.vmap(positions)(ids)
    source = jnp.arange(N_EXPERT, dtype=jnp.int32)[:, None]
    flat = (ids * SLOTS + source * CAP + slot).reshape(-1).astype(jnp.int32)
    token = jnp.repeat(jnp.arange(TOKENS, dtype=jnp.int32), K)
    affinity = jax.nn.sigmoid(router_logits.astype(jnp.float32))
    total = jnp.sum(affinity, axis=1, keepdims=True)
    gate = routed_scale * affinity / total
    keep_f = keep.astype(jnp.float32)
    weight = (gate * keep_f).astype(jnp.bfloat16).astype(jnp.float32)
    table = jnp.full((EXPERTS * SLOTS,), TOKENS, jnp.int32).at[flat].set(token).reshape(EXPERTS, SLOTS)
    weight_table = jnp.zeros((EXPERTS * SLOTS,), jnp.float32).at[flat].set(weight.reshape(-1)).reshape(EXPERTS, SLOTS)
    padded = jnp.concatenate([grad_out, jnp.zeros((1, D), jnp.bfloat16)], axis=0)

    def step(accum, expert):
        index = table[expert]
        rows = padded[index]
        hidden_grad = jnp.dot(rows, w_down[expert].T, preferred_element_type=jnp.float32)
        gate_pre = saved_gate[expert].T.astype(jnp.float32)
        up_pre = saved_up[expert].T.astype(jnp.float32)
        sig = jax.nn.sigmoid(gate_pre)
        act = gate_pre * sig
        act_grad = sig * (1.0 + gate_pre * (1.0 - sig))
        gate_grad = (hidden_grad * up_pre * act_grad).astype(jnp.bfloat16)
        up_grad = (hidden_grad * act).astype(jnp.bfloat16)
        score = jnp.sum(hidden_grad * act * up_pre, axis=1).astype(jnp.bfloat16)
        copy_grad = (jnp.dot(gate_grad, w_gate[expert].T, preferred_element_type=jnp.float32)
                     + jnp.dot(up_grad, w_up[expert].T, preferred_element_type=jnp.float32)).astype(jnp.bfloat16)
        accum = accum.at[index].add(weight_table[expert][:, None] * copy_grad.astype(jnp.float32))
        return accum, score

    accum, scores = lax.scan(step, jnp.zeros((TOKENS + 1, D), jnp.float32), jnp.arange(EXPERTS, dtype=jnp.int32))
    grad_tokens = accum[:TOKENS].astype(jnp.bfloat16)
    copy_score = scores.reshape(-1)[flat].astype(jnp.float32).reshape(TOKENS, K)
    weight_grad = keep_f * copy_score
    mixed = jnp.sum(weight_grad * affinity, axis=1, keepdims=True)
    affinity_grad = routed_scale * (weight_grad / total - mixed / (total * total))
    router_grad = affinity_grad * affinity * (1.0 - affinity)
    return grad_tokens, router_grad
```

```python
import math

import jax
import jax.numpy as jnp
from jax import lax
from jax.sharding import PartitionSpec as P

routed_scale = 2.5
lanes = 128


def sub_axes(experts):
    cores = 2 if experts % 2 == 0 else 1
    chips = experts // cores
    y = max(1, math.isqrt(max(1, chips // 2)))
    while chips % y:
        y -= 1
    return chips // y, y, cores


class Ring:
    def __init__(self, sizes, which):
        self.sizes, self.which, self.size = sizes, which, sizes[which]

    def move(self, value, step):
        zs, ys, cs = self.sizes
        pairs = []
        for z in range(zs):
            for y in range(ys):
                for c in range(cs):
                    to = [z, y, c]
                    to[self.which] = (to[self.which] + step) % self.size
                    pairs.append(((z * ys + y) * cs + c, (to[0] * ys + to[1]) * cs + to[2]))
        return lax.ppermute(value, "expert", pairs)

    def gather(self, value):
        size, half = self.size, self.size // 2
        blocks = [value] + [None] * (size - 1)
        if size == 2:
            blocks[1] = self.move(value, 1)
            return blocks
        down = up = value
        for d in range(1, half + size % 2):
            down, up = self.move(down, -1), self.move(up, 1)
            blocks[d], blocks[size - d] = down, up
        if size % 2 == 0:
            cut = value.shape[-1] // (2 * lanes) * lanes
            blocks[half] = jnp.concatenate(
                [self.move(down[..., :cut], -1), self.move(up[..., cut:], 1)], axis=-1
            )
        return blocks

    def reduce(self, blocks):
        size, half = self.size, self.size // 2
        total = blocks[0].astype(jnp.float32)
        if size == 1:
            return total
        if size == 2:
            return total + self.move(blocks[1], 1).astype(jnp.float32)
        cut = blocks[0].shape[-1] // (2 * lanes) * lanes
        for direction in (1, -1):
            last = half if size % 2 else half - 1
            held = blocks[direction * last % size]
            if size % 2 == 0:
                far = blocks[half]
                if direction == 1:
                    got = self.move(far[..., :cut], 1).astype(jnp.float32)
                    near = (got + held[..., :cut].astype(jnp.float32)).astype(held.dtype)
                    held = jnp.concatenate([near, held[..., cut:]], axis=-1)
                else:
                    got = self.move(far[..., cut:], -1).astype(jnp.float32)
                    near = (got + held[..., cut:].astype(jnp.float32)).astype(held.dtype)
                    held = jnp.concatenate([held[..., :cut], near], axis=-1)
            for d in range(last - 1, 0, -1):
                got = self.move(held, direction).astype(jnp.float32)
                held = (got + blocks[direction * d % size].astype(jnp.float32)).astype(held.dtype)
            total = total + self.move(held, direction).astype(jnp.float32)
        return total


def shifted(value, axis, size, step):
    return lax.ppermute(value, axis, [(i, (i + step) % size) for i in range(size)])


def whole_over(value, axis):
    size = lax.axis_size(axis)
    index = lax.axis_index(axis)
    part = value.shape[0]
    result = jnp.zeros((part * size,) + value.shape[1:], value.dtype)
    result = lax.dynamic_update_slice(result, value, (index * part, 0))
    for step in range(1, size):
        got = shifted(value, axis, size, step)
        origin = lax.rem(index - step + size, size)
        result = lax.dynamic_update_slice(result, got, (origin * part, 0))
    return result


def contract(grads, columns):
    return lax.dot_general(
        grads, columns, (((0,), (1,)), ((), ())), preferred_element_type=jnp.float32
    )


def on_device(
    grad_out, expert_ids, keep, router_logits, w_gate, w_up, w_down, saved_gate, saved_up
):
    experts = lax.axis_size("expert")
    dp = lax.axis_size("dp")
    me = lax.axis_index("expert")
    tok_rows, topk = expert_ids.shape
    slots = saved_gate.shape[2]
    capacity = slots // experts
    width_part = grad_out.shape[1]
    sizes = zs, ys, cs = sub_axes(experts)
    ring_z, ring_y, ring_c = (Ring(sizes, i) for i in range(3))
    cut = -(-width_part * 4 // (7 * lanes)) * lanes

    place = jnp.arange(slots, dtype=jnp.int32)
    block = place // capacity
    dz, dc, dy = block // (cs * ys), block // ys % cs, block % ys
    my_z, my_y, my_c = me // (ys * cs), me // cs % ys, me % cs
    source = ((my_z + dz) % zs * ys + (my_y + dy) % ys) * cs + (my_c + dc) % cs
    slot_of = source * capacity + place % capacity
    reorder = (jnp.arange(slots, dtype=jnp.int32)[:, None] == slot_of[None, :]).astype(jnp.bfloat16)
    gate_pre = whole_over(jnp.dot(saved_gate[0], reorder), "dp")
    up_pre = whole_over(jnp.dot(saved_up[0], reorder), "dp")

    affinity = jax.nn.sigmoid(router_logits)
    total = jnp.sum(affinity, axis=1, keepdims=True)
    gate = routed_scale * affinity / total
    keep_f = keep.astype(jnp.float32)
    weight = (gate * keep_f).astype(jnp.bfloat16)
    extra = -(-2 * topk // lanes) * lanes
    info = jnp.concatenate([expert_ids.astype(jnp.bfloat16), weight], axis=1)
    info = jnp.pad(info, ((0, 0), (0, extra - 2 * topk)))

    first = jnp.stack(ring_y.gather(grad_out[:, :cut]))
    first = ring_z.gather(first)
    first = [ring_c.gather(part) for part in first]
    second = ring_z.gather(jnp.concatenate([grad_out[:, cut:], info], axis=1))
    second = [[list(t) for t in zip(*[ring_c.gather(p) for p in ring_y.gather(part)])] for part in second]

    tail = width_part - cut
    infos = jnp.stack([p[:, tail:] for by_c in second for by_y in by_c for p in by_y])
    hit = infos[..., :topk] == me.astype(jnp.bfloat16)
    mine = jnp.any(hit, axis=2)
    mine_weight = jnp.sum(
        jnp.where(hit, infos[..., topk : 2 * topk].astype(jnp.float32), 0.0), axis=2
    )
    before = jnp.arange(tok_rows)[:, None] < jnp.arange(tok_rows)[None, :]
    position = jnp.dot(
        mine.astype(jnp.bfloat16), before.astype(jnp.bfloat16), preferred_element_type=jnp.float32
    ).astype(jnp.int32)
    route = mine[:, None, :] & (
        position[:, None, :] == jnp.arange(capacity, dtype=jnp.int32)[None, :, None]
    )
    combine = jnp.where(route, mine_weight[:, None, :], 0.0).astype(jnp.bfloat16)
    route = route.astype(jnp.bfloat16)

    def rows_of(pieces):
        return lax.dot_general(
            route, pieces, (((2,), (1,)), ((0,), (0,))), preferred_element_type=jnp.float32
        ).astype(jnp.bfloat16).reshape(slots, -1)

    def down(rows, span):
        return lax.dot_general(
            w_down[0, :, span], rows, (((1,), (1,)), ((), ())), preferred_element_type=jnp.float32
        )

    head_span, tail_span = slice(0, cut), slice(cut, width_part)
    first = jnp.concatenate([p for by_c in first for p in by_c])
    second = jnp.stack([p[:, :tail] for by_c in second for by_y in by_c for p in by_y])
    first, second, gate_pre, up_pre = lax.optimization_barrier((first, second, gate_pre, up_pre))
    partial = down(rows_of(first), head_span) + down(rows_of(second), tail_span)
    sent = partial.astype(jnp.bfloat16)
    hidden = partial
    for shift in range(1, dp):
        hidden = hidden + shifted(sent, "dp", dp, shift).astype(jnp.float32)

    gate_f = gate_pre.astype(jnp.float32)
    up_f = up_pre.astype(jnp.float32)
    sig = jax.nn.sigmoid(gate_f)
    act = gate_f * sig
    act_grad = sig * (1.0 + gate_f * (1.0 - sig))
    gate_grad = (hidden * up_f * act_grad).astype(jnp.bfloat16)
    up_grad = (hidden * act).astype(jnp.bfloat16)
    score = jnp.sum(hidden * act * up_f, axis=0).astype(jnp.bfloat16).reshape(experts, capacity)
    mine_score = jnp.sum(route.astype(jnp.float32) * score.astype(jnp.float32)[:, :, None], axis=1)
    scores = jnp.where(hit, mine_score[:, :, None], 0.0).astype(jnp.bfloat16)
    scores = jnp.pad(scores, ((0, 0), (0, 0), (0, extra - topk)))

    def shares(span, gate_grad, up_grad):
        copy_grad = contract(gate_grad, w_gate[0, span]) + contract(up_grad, w_up[0, span])
        copy_grad = copy_grad.astype(jnp.bfloat16).reshape(experts, capacity, -1)
        return lax.dot_general(
            combine, copy_grad, (((1,), (1,)), ((0,), (0,))), preferred_element_type=jnp.float32
        ).astype(jnp.bfloat16)

    def over_cores(share):
        share = share.reshape(zs, cs, ys, tok_rows, share.shape[-1])
        return ring_c.reduce([share[:, c] for c in range(cs)]).astype(jnp.bfloat16)

    lead = shares(head_span, gate_grad, up_grad)
    lead, gate_grad, up_grad = lax.optimization_barrier((lead, gate_grad, up_grad))
    lead = over_cores(lead)
    last = over_cores(jnp.concatenate([shares(tail_span, gate_grad, up_grad), scores], axis=2))
    lead = ring_z.reduce([lead[z] for z in range(zs)]).astype(jnp.bfloat16)
    lead = ring_y.reduce([lead[y] for y in range(ys)])
    last = ring_y.reduce([last[:, y] for y in range(ys)]).astype(jnp.bfloat16)
    last = ring_z.reduce([last[z] for z in range(zs)])
    grad_tokens = jnp.concatenate([lead, last[:, :tail]], axis=1).astype(jnp.bfloat16)

    weight_grad = keep_f * last[:, tail : tail + topk]
    mixed = jnp.sum(weight_grad * affinity, axis=1, keepdims=True)
    affinity_grad = routed_scale * (weight_grad / total - mixed / (total * total))
    router_grad = affinity_grad * affinity * (1.0 - affinity)
    return (grad_tokens, router_grad)


def solution(mesh):
    in_specs = (
        P("expert", "dp"),
        P("expert", None),
        P("expert", None),
        P("expert", None),
        P("expert", "dp", None),
        P("expert", "dp", None),
        P("expert", None, "dp"),
        P("expert", "dp", None),
        P("expert", "dp", None),
    )
    out_specs = (P("expert", "dp"), P("expert", None))
    return jax.shard_map(
        on_device, mesh=mesh, in_specs=in_specs, out_specs=out_specs, check_vma=False
    )
```
